1024 devices in a mesh: grp: 64 (over y_lo, z, core), sp: 16 (over x, y_hi).
Axes of the slice: x: 8, y: 8 (y_hi: 2, y_lo: 4; y = y_hi * 4 + y_lo), z: 8, core: 2. Of those that a mesh axis runs over, the one named last changes fastest.
Arguments:
- acts: bfloat16 [1024, 16, 16, 728], P('grp', 'sp'), may hold values from -6 to 6
- cotangent: bfloat16 [1024, 16, 16, 728], P(('grp', 'sp')), may hold values from -6 to 6
- depth_kernel: float32 [3, 3, 728], replicated, may hold values from -2 to 2
- point_weight: bfloat16 [728, 728], replicated, may hold values from -0.21875 to 0.21875
- batch_norm_gain: float32 [728], replicated, may hold values from 0.5 to 2
- norm_shift_bias: float32 [728], replicated, may hold values from -1 to 1
Outputs:
- block_out: bfloat16 [1024, 16, 16, 728], P(('grp', 'sp'))
- input_grad: bfloat16 [1024, 16, 16, 728], P('grp', 'sp')
- weight_grad: float32 [529984], P('sp')
The draws below stay inside these ranges and needn't reach their ends.
All inputs are finite; a program needn't handle non-finite values.
Results may differ from the reference program's by a relative error of at most 0.018.
Values may be sent and summed in bfloat16 or wider, within the bound.
No kernel may reach another device: no remote copies, remote signals or barrier semaphores. Data moves between devices by JAX's collectives and lax.ppermute only.
A program may use at most 32 MiB of HBM per device.

```python
import math
import jax
import jax.numpy as jnp
from jax import lax

C = 728
COLS = 16
ROWS = 16
BATCH = 1024
N_GRP = 64
N_SP = 16


def block_scale(stream_key, extent, pieces, least, largest):
    loudness, own = 1.0, jax.random.fold_in(stream_key, 6)
    for axis_at, blocks in pieces:
        draws = jnp.exp(jax.random.uniform(jax.random.fold_in(own, axis_at), (blocks,), jnp.float32, least / len(pieces), largest / len(pieces)))
        loudness = loudness * jnp.repeat(draws, extent[axis_at] // blocks).reshape([-1 if axis == axis_at else 1 for axis in range(len(extent))])
    return loudness


def centred(stream_key, shape, deviation, bound, cuts=(), dtype=jnp.bfloat16):
    array = deviation * jax.random.normal(stream_key, shape, jnp.float32)
    if cuts:
        array = array * block_scale(stream_key, shape, cuts, -0.22, 0.18)
    return jnp.clip(array, -bound, bound).astype(dtype)


def setup_inputs(seed: int = 0) -> dict:
    seeds = jax.random.split(jax.random.key(seed), 7)
    acts = centred(seeds[0], (BATCH, ROWS, COLS, C), 1.0, 6.0, ((0, 64), (1, 16)))
    cotangent = centred(seeds[1], (BATCH, ROWS, COLS, C), 1.0, 6.0, ((0, 1024),))
    depth_kernel = centred(seeds[2], (3, 3, C), 9 ** -0.5, 2.0, (), jnp.float32)
    point_weight = centred(seeds[3], (C, C), C ** -0.5, 0.21875)
    batch_norm_gain = jnp.clip(jnp.exp(jax.random.uniform(seeds[4], (C,), jnp.float32, math.log(0.5), math.log(2.0))), 0.5, 2.0)
    norm_shift_bias = jnp.clip(jax.random.uniform(seeds[5], (C,), jnp.float32, -1.0, 1.0), -1.0, 1.0)
    return {"acts": acts, "cotangent": cotangent, "depth_kernel": depth_kernel, "point_weight": point_weight, "batch_norm_gain": batch_norm_gain, "norm_shift_bias": norm_shift_bias}


def depth_forward(field, filter_weight):
    rows = field.shape[1]
    cols = field.shape[2]
    padded = jnp.pad(field, ((0, 0), (1, 1), (1, 1), (0, 0)))
    total = jnp.zeros(field.shape, jnp.float32)
    for i in range(3):
        for j in range(3):
            total = total + padded[:, i:i + rows, j:j + cols, :] * filter_weight[i, j]
    return total

def depth_backward(field, filter_weight):
    rows = field.shape[1]
    cols = field.shape[2]
    padded = jnp.pad(field, ((0, 0), (1, 1), (1, 1), (0, 0)))
    total = jnp.zeros(field.shape, jnp.float32)
    for i in range(3):
        for j in range(3):
            total = total + padded[:, 2 - i:2 - i + rows, 2 - j:2 - j + cols, :] * filter_weight[i, j]
    return total

def one_group(carry, pair, depth_kernel, point_weight, batch_norm_gain, norm_shift_bias):
    inputs, grads = pair
    channel_count = inputs.shape[-1]
    sample_count = inputs.shape[0]
    input_single_precision = inputs.astype(jnp.float32)
    hidden = jnp.maximum(input_single_precision, 0.0)
    depthed = depth_forward(hidden, depth_kernel).astype(jnp.bfloat16)
    flat_d = depthed.reshape(-1, channel_count)
    element_count = flat_d.shape[0]
    projected_output = jnp.dot(flat_d, point_weight, preferred_element_type=jnp.float32)
    batch_mean = lax.optimization_barrier(jnp.sum(projected_output, axis=0)) / element_count
    var = lax.optimization_barrier(jnp.sum(projected_output * projected_output, axis=0)) / element_count - batch_mean * batch_mean
    inverse_deviation = lax.rsqrt(var + 1e-05)
    normalized_input = (projected_output - batch_mean) * inverse_deviation
    layer_outputs = (input_single_precision.reshape(-1, channel_count) + batch_norm_gain * normalized_input + norm_shift_bias).astype(jnp.bfloat16)
    gfloat = grads.astype(jnp.float32).reshape(-1, channel_count)
    scaled_output = gfloat * batch_norm_gain
    leading_layer = lax.optimization_barrier(jnp.sum(scaled_output, axis=0)) / element_count
    second_layer = lax.optimization_barrier(jnp.sum(scaled_output * normalized_input, axis=0)) / element_count
    projected_gradient = (inverse_deviation * (scaled_output - leading_layer - normalized_input * second_layer)).astype(jnp.bfloat16)
    per_device = flat_d.astype(jnp.float32).reshape(sample_count, -1, channel_count)
    per_group = projected_gradient.astype(jnp.float32).reshape(sample_count, -1, channel_count)
    term_list = jnp.einsum('ayu,ayq->auq', per_device, per_group).astype(jnp.bfloat16)
    term_list = lax.optimization_barrier(term_list).astype(jnp.float32)
    local_weight = lax.optimization_barrier(jnp.sum(term_list, axis=0))
    ddepth = jnp.dot(projected_gradient, point_weight.T, preferred_element_type=jnp.float32).reshape(inputs.shape)
    dhidden = depth_backward(ddepth, depth_kernel)
    dinput = (gfloat.reshape(inputs.shape) + jnp.where(inputs > 0, dhidden, 0.0)).astype(jnp.bfloat16)
    return (carry + local_weight, (layer_outputs.reshape(inputs.shape), dinput))

def reference(acts, cotangent, depth_kernel, point_weight, batch_norm_gain, norm_shift_bias):
    channel_count = acts.shape[-1]
    shape_g = (N_GRP, N_SP) + acts.shape[1:]
    xs = (acts.reshape(shape_g), cotangent.reshape(shape_g))

    def stepper(carry, pair):
        return one_group(carry, pair, depth_kernel, point_weight, batch_norm_gain, norm_shift_bias)
    wsum, pair_out = lax.scan(stepper, jnp.zeros((channel_count, channel_count), jnp.float32), xs)
    block_out = pair_out[0].reshape(acts.shape)
    input_grad = pair_out[1].reshape(acts.shape)
    return (block_out, input_grad, wsum.reshape(-1))
```

```python
import jax
import jax.numpy as jnp
import numpy as np
from jax import lax
from jax.experimental import pallas as pl
from jax.experimental.pallas import tpu as pltpu
from jax.sharding import Mesh, PartitionSpec as P

BF = jnp.bfloat16
F32 = jnp.float32
SP = ("x", "yh")
LINE = ("yl", "z")
GRP = ("yl", "z", "core")
VMEM = pl.BlockSpec(memory_space=pltpu.VMEM)


def call(kernel, outs, name, flops, *args):
    size = sum(a.size * a.dtype.itemsize for a in args)
    size += sum(int(np.prod(o.shape)) * o.dtype.itemsize for o in outs)
    return pl.pallas_call(
        kernel,
        out_shape=outs,
        in_specs=[VMEM] * len(args),
        out_specs=[VMEM] * len(outs),
        cost_estimate=pl.CostEstimate(flops=flops, bytes_accessed=size, transcendentals=0),
        name=name,
    )(*args)


def spans(width, step):
    return [(a, min(a + step, width)) for a in range(0, width, step)]


def shifted(field):
    zero = jnp.zeros_like(field[:, :1, :])
    left = jnp.concatenate([zero, field[:, :-1, :]], axis=1)
    right = jnp.concatenate([field[:, 1:, :], zero], axis=1)
    return left, field, right


def nine_taps(field, taps, flip):
    rows = field.shape[0]
    near = shifted(field)
    out = []
    for r in range(rows):
        total = None
        for i in range(3):
            src = r + (1 - i if flip else i - 1)
            if src < 0 or src >= rows:
                continue
            for j in range(3):
                part = near[2 - j if flip else j][src] * taps[i, j : j + 1, :]
                total = part if total is None else total + part
        out.append(total)
    return out


def forward_kernel(x_ref, g_ref, k_ref, w_ref, d_ref, p_ref, s_ref):
    rows, cols, width = x_ref.shape
    for a, b in spans(width, 128):
        h = jnp.maximum(x_ref[:, :, a:b].astype(F32), 0.0)
        for r, line in enumerate(nine_taps(h, k_ref[:, :, a:b], False)):
            d_ref[r * cols : (r + 1) * cols, a:b] = line.astype(BF)
    p_ref[...] = jnp.dot(d_ref[...], w_ref[...], preferred_element_type=F32)
    for a, b in spans(width, 128):
        p = p_ref[:, a:b]
        g = g_ref[:, :, a:b].astype(F32).reshape(rows * cols, b - a)
        sums = [jnp.sum(v, axis=0, keepdims=True) for v in (p, p * p, g, g * p)]
        stats = jnp.concatenate(sums, axis=0)
        for k in range(s_ref.shape[0]):
            s_ref[k, :, a:b] = stats


def pick_kernel(d_ref, i_ref, t_ref):
    width = d_ref.shape[1]
    chan = lax.broadcasted_iota(jnp.int32, (t_ref.shape[0], width), 1)
    pick = jnp.where(chan == i_ref[...], 1.0, 0.0).astype(BF)
    t = lax.dot_general(pick, d_ref[...], (((1,), (1,)), ((), ())), preferred_element_type=F32)
    t_ref[...] = t.astype(BF)


def project_kernel(count, s_ref, p_ref, g_ref, gain_ref, t_ref, c_ref, dp_ref, o_ref):
    rows, cols, width = g_ref.shape
    for a, b in spans(width, 128):
        stats = s_ref[0, :, a:b]
        for k in range(1, s_ref.shape[0]):
            stats = stats + s_ref[k, :, a:b]
        gain = gain_ref[:, a:b]
        mean = stats[0:1] / count
        var = stats[1:2] / count - mean * mean
        rstd = lax.rsqrt(var + 1e-05)
        lead = gain * stats[2:3] / count
        second = gain * rstd * (stats[3:4] - mean * stats[2:3]) / count
        c_ref[0:1, a:b] = mean
        c_ref[1:2, a:b] = rstd
        g = g_ref[:, :, a:b].astype(F32).reshape(rows * cols, b - a)
        xhat = (p_ref[:, a:b] - mean) * rstd
        dp_ref[:, a:b] = (rstd * (g * gain - lead - xhat * second)).astype(BF)
    half = t_ref.shape[0] // 2
    other = jnp.dot(t_ref[half:, :], dp_ref[...], preferred_element_type=F32).astype(BF)
    n, part, _ = o_ref.shape
    for k in range(n):
        o_ref[k] = other[k * part : (k + 1) * part, :]


def input_kernel(dp_ref, t_ref, w_ref, k_ref, g_ref, x_ref, m_ref, di_ref, dd_ref):
    rows, cols, width = g_ref.shape
    half = t_ref.shape[0] // 2
    m_ref[...] = jnp.dot(t_ref[:half, :], dp_ref[...], preferred_element_type=F32)
    dd_ref[...] = lax.dot_general(
        dp_ref[...], w_ref[...], (((1,), (1,)), ((), ())), preferred_element_type=F32
    )
    for a, b in spans(width, 128):
        dd = dd_ref[:, a:b].reshape(rows, cols, b - a)
        for r, line in enumerate(nine_taps(dd, k_ref[:, :, a:b], True)):
            kept = jnp.where(x_ref[r, :, a:b].astype(F32) > 0, line, 0.0)
            di_ref[r, :, a:b] = (g_ref[r, :, a:b].astype(F32) + kept).astype(BF)


def output_kernel(x_ref, p_ref, c_ref, gain_ref, bias_ref, o_ref):
    rows, cols, width = x_ref.shape
    for a, b in spans(width, 128):
        xhat = (p_ref[:, a:b] - c_ref[0:1, a:b]) * c_ref[1:2, a:b]
        norm = (gain_ref[:, a:b] * xhat).reshape(rows, cols, b - a)
        out = x_ref[:, :, a:b].astype(F32) + norm + bias_ref[:, a:b]
        o_ref[:, :, a:b] = out.astype(BF)


def pack_kernel(m_ref, r_ref, di_ref, o_ref):
    n, cols, _ = di_ref.shape
    part = m_ref.shape[0] // n
    for k in range(n):
        rows = slice(k * part, (k + 1) * part)
        o_ref[k, :part, :] = (m_ref[rows, :] + r_ref[k].astype(F32)).astype(BF)
        o_ref[k, part:, :] = di_ref[k]


def slice_kernel(b_ref, o_ref):
    n = b_ref.shape[0]
    lines, per, width = o_ref.shape
    part = b_ref.shape[1] - 16
    total = b_ref[0, :part, :].astype(F32)
    for k in range(1, n):
        total = total + b_ref[k, :part, :].astype(F32)
    for k in range(lines):
        for q in range(per):
            r = k * per + q
            if r < part:
                o_ref[k, q : q + 1, :] = total[r : r + 1, :]
            else:
                o_ref[k, q : q + 1, :] = jnp.zeros((1, width), F32)


def out(shape, dtype):
    return jax.ShapeDtypeStruct(shape, dtype)


def channel_table(width, parts):
    per = -(-(width * width // parts) // width)
    half = -(-(per // 2 + 1) // 8) * 8
    table = np.full((2, parts, half), -1, np.int32)
    for c in range(2):
        for k in range(parts):
            first = (width * k) // parts
            for r in range(half):
                row = 2 * r + c
                if row < per and first + row < width:
                    table[c, k, r] = first + row
    return table.reshape(2, parts * half), half, per


def body(acts, cotangent, depth_kernel, point_weight, gain, bias):
    n = lax.axis_size(SP)
    lines = lax.axis_size(LINE)
    copies = lax.axis_size(GRP)
    _, rows, cols, width = cotangent.shape
    places = rows * cols
    count = places * n
    table, half, per = channel_table(width, n)
    core = lax.axis_index("core")
    mine = jnp.where(core == 0, table.reshape(-1), table[::-1].reshape(-1))[:, None]
    gain = gain[None]
    bias = bias[None]
    g = cotangent[0]

    x = lax.all_to_all(acts[:, 0], SP, 0, 0, tiled=True)
    d, p, stats = call(
        forward_kernel,
        [out((places, width), BF), out((places, width), F32), out((n, 4, width), F32)],
        "forward", 2 * places * width * width, x, g, depth_kernel, point_weight,
    )
    stats = lax.all_to_all(stats, SP, 0, 0, tiled=True)
    (picked,) = call(
        pick_kernel, [out((2 * n * half, places), BF)], "pick",
        4 * places * width * n * half, d, mine,
    )
    coefs, dp, other = call(
        lambda *refs: project_kernel(float(count), *refs),
        [out((2, width), F32), out((places, width), BF), out((n, half, width), BF)],
        "project", 2 * places * width * n * half, stats, p, g, gain, picked,
    )
    other = lax.ppermute(other, "core", [(0, 1), (1, 0)])
    own, dinput, _ = call(
        input_kernel,
        [out((n * half, width), F32), out((rows, cols, width), BF), out((places, width), F32)],
        "input", 4 * places * width * width, dp, picked, point_weight, depth_kernel, g, x,
    )
    (packed,) = call(
        pack_kernel, [out((n, half + cols, width), BF)], "pack", n * half * width, own, other, dinput
    )
    packed = lax.all_to_all(packed, SP, 0, 0, tiled=True)
    (block_out,) = call(
        output_kernel, [out((rows, cols, width), BF)], "output", 4 * places * width,
        x, p, coefs, gain, bias,
    )
    each = -(-half // lines)
    (pieces,) = call(
        slice_kernel, [out((lines, each, width), F32)], "slice", n * half * width, packed
    )
    pieces = lax.all_to_all(pieces, LINE, 0, 0, tiled=True)
    summed = jnp.broadcast_to(jnp.sum(pieces, axis=0), (copies, each, width))
    whole = lax.all_to_all(summed, GRP, 0, 0, tiled=True)
    whole = whole.reshape(lines, 2, each, width).swapaxes(1, 2).reshape(-1)
    span = width * width // n
    shift = (lax.axis_index(SP) * span) % width
    if (2 * span) % width == 0:
        odd = shift != 0
        weight_grad = jnp.where(odd, whole[width // 2 : width // 2 + span], whole[:span])
    else:
        weight_grad = lax.dynamic_slice(whole, (shift,), (span,))
    input_grad = packed[:, half:, :][:, None]
    return block_out[None], input_grad, weight_grad


def solution(mesh):
    sizes = (4, mesh.shape["grp"] // 8, 2, mesh.shape["sp"] // 2, 2)
    fine = Mesh(mesh.devices.reshape(sizes), ("yl", "z", "core", "x", "yh"))
    in_specs = (P(GRP, SP, None, None), P(GRP + SP, None, None, None), P(), P(), P(), P())
    out_specs = (P(GRP + SP, None, None, None), P(GRP, SP, None, None), P(SP))
    return jax.shard_map(body, mesh=fine, in_specs=in_specs, out_specs=out_specs, check_vma=False)
```

```python
import jax
import jax.numpy as jnp
import numpy as np
from jax import lax
from jax.experimental import pallas as pl
from jax.experimental.pallas import tpu as pltpu
from jax.sharding import Mesh, PartitionSpec as P

BF = jnp.bfloat16
F32 = jnp.float32
SP = ("x", "yh")
LINE = ("yl", "z")
GRP = ("yl", "z", "core")
VMEM = pl.BlockSpec(memory_space=pltpu.VMEM)


def held_in(a, space):
    return pltpu.with_memory_space_constraint(a, space)


def call(kernel, outs, name, flops, *args, far=()):
    size = sum(a.size * a.dtype.itemsize for a in args)
    size += sum(int(np.prod(o.shape)) * o.dtype.itemsize for o in outs)
    return pl.pallas_call(
        kernel,
        out_shape=outs,
        in_specs=[VMEM] * len(args),
        out_specs=[VMEM] * len(outs),
        cost_estimate=pl.CostEstimate(flops=flops, bytes_accessed=size, transcendentals=0),
        compiler_params=pltpu.CompilerParams(vmem_limit_bytes=16 * 2**20),
        name=name,
    )(*[held_in(a, pltpu.HBM if k in far else pltpu.VMEM) for k, a in enumerate(args)])


def spans(width, step):
    return [(a, min(a + step, width)) for a in range(0, width, step)]


def shifted(field):
    zero = jnp.zeros_like(field[:, :1, :])
    left = jnp.concatenate([zero, field[:, :-1, :]], axis=1)
    right = jnp.concatenate([field[:, 1:, :], zero], axis=1)
    return left, field, right


def nine_taps(field, taps, flip):
    rows = field.shape[0]
    near = shifted(field)
    out = []
    for r in range(rows):
        total = None
        for i in range(3):
            src = r + (1 - i if flip else i - 1)
            if src < 0 or src >= rows:
                continue
            for j in range(3):
                part = near[2 - j if flip else j][src] * taps[i, j : j + 1, :]
                total = part if total is None else total + part
        out.append(total)
    return out


def stage_kernel(*refs):
    half = len(refs) // 2
    for src, dst in zip(refs[:half], refs[half:]):
        dst[...] = src[...]


def forward_kernel(x_ref, g_ref, k_ref, w_ref, d_ref, p_ref, s_ref):
    rows, cols, width = x_ref.shape
    for a, b in spans(width, 128):
        h = jnp.maximum(x_ref[:, :, a:b].astype(F32), 0.0)
        for r, line in enumerate(nine_taps(h, k_ref[:, :, a:b], False)):
            d_ref[r * cols : (r + 1) * cols, a:b] = line.astype(BF)
    p_ref[...] = jnp.dot(d_ref[...], w_ref[...], preferred_element_type=F32)
    for a, b in spans(width, 128):
        p = p_ref[:, a:b]
        g = g_ref[:, :, a:b].astype(F32).reshape(rows * cols, b - a)
        sums = [jnp.sum(v, axis=0, keepdims=True) for v in (p, p * p, g, g * p)]
        stats = jnp.concatenate(sums, axis=0)
        for k in range(s_ref.shape[0]):
            s_ref[k, :, a:b] = stats


def pick_kernel(parts, d_ref, t_ref):
    width = d_ref.shape[1]
    lines = t_ref.shape[0]
    part = lines // 2 // parts
    per = -(-width // parts)
    core = lax.axis_index("core")
    line = lax.broadcasted_iota(jnp.int32, (lines, 1), 0)
    other = line >= lines // 2
    line = jnp.where(other, line - lines // 2, line)
    slot = (line * (65536 // part + 1)) >> 16
    row = 2 * (line - part * slot) + jnp.where(other, 1 - core, core)
    source = ((slot * (2 * width // parts)) >> 1) + row
    source = jnp.where(row < per, source, -1)
    chan = lax.broadcasted_iota(jnp.int32, (lines, width), 1)
    pick = jnp.where(chan == source, 1.0, 0.0).astype(BF)
    t = lax.dot_general(pick, d_ref[...], (((1,), (1,)), ((), ())), preferred_element_type=F32)
    t_ref[...] = t.astype(BF)


def project_kernel(count, s_ref, p_ref, g_ref, gain_ref, t_ref, c_ref, dp_ref, o_ref):
    rows, cols, width = g_ref.shape
    for a, b in spans(width, 128):
        stats = s_ref[0, :, a:b]
        for k in range(1, s_ref.shape[0]):
            stats = stats + s_ref[k, :, a:b]
        gain = gain_ref[:, a:b]
        mean = stats[0:1] / count
        var = stats[1:2] / count - mean * mean
        rstd = lax.rsqrt(var + 1e-05)
        lead = gain * stats[2:3] / count
        second = gain * rstd * (stats[3:4] - mean * stats[2:3]) / count
        c_ref[0:1, a:b] = mean
        c_ref[1:2, a:b] = rstd
        g = g_ref[:, :, a:b].astype(F32).reshape(rows * cols, b - a)
        xhat = (p_ref[:, a:b] - mean) * rstd
        dp_ref[:, a:b] = (rstd * (g * gain - lead - xhat * second)).astype(BF)
    half = t_ref.shape[0] // 2
    other = jnp.dot(t_ref[half:, :], dp_ref[...], preferred_element_type=F32).astype(BF)
    n, part, _ = o_ref.shape
    for k in range(n):
        o_ref[k] = other[k * part : (k + 1) * part, :]


def input_kernel(dp_ref, t_ref, w_ref, k_ref, g_ref, x_ref, m_ref, di_ref, dd_ref):
    rows, cols, width = g_ref.shape
    half = t_ref.shape[0] // 2
    m_ref[...] = jnp.dot(t_ref[:half, :], dp_ref[...], preferred_element_type=F32)
    dd_ref[...] = lax.dot_general(
        dp_ref[...], w_ref[...], (((1,), (1,)), ((), ())), preferred_element_type=F32
    )
    for a, b in spans(width, 128):
        dd = dd_ref[:, a:b].reshape(rows, cols, b - a)
        for r, line in enumerate(nine_taps(dd, k_ref[:, :, a:b], True)):
            kept = jnp.where(x_ref[r, :, a:b].astype(F32) > 0, line, 0.0)
            di_ref[r, :, a:b] = (g_ref[r, :, a:b].astype(F32) + kept).astype(BF)


def output_kernel(x_ref, p_ref, c_ref, gain_ref, bias_ref, o_ref):
    rows, cols, width = x_ref.shape
    for a, b in spans(width, 128):
        xhat = (p_ref[:, a:b] - c_ref[0:1, a:b]) * c_ref[1:2, a:b]
        norm = (gain_ref[:, a:b] * xhat).reshape(rows, cols, b - a)
        out = x_ref[:, :, a:b].astype(F32) + norm + bias_ref[:, a:b]
        o_ref[:, :, a:b] = out.astype(BF)


def pack_kernel(m_ref, r_ref, di_ref, o_ref):
    n, cols, _ = di_ref.shape
    part = m_ref.shape[0] // n
    for k in range(n):
        rows = slice(k * part, (k + 1) * part)
        o_ref[k, :part, :] = (m_ref[rows, :] + r_ref[k].astype(F32)).astype(BF)
        o_ref[k, part:, :] = di_ref[k]


def slice_kernel(b_ref, o_ref):
    n = b_ref.shape[0]
    lines, per, width = o_ref.shape
    part = b_ref.shape[1] - 16
    total = b_ref[0, :part, :].astype(F32)
    for k in range(1, n):
        total = total + b_ref[k, :part, :].astype(F32)
    for k in range(lines):
        for q in range(per):
            r = k * per + q
            if r < part:
                o_ref[k, q : q + 1, :] = total[r : r + 1, :]
            else:
                o_ref[k, q : q + 1, :] = jnp.zeros((1, width), F32)


def copies_kernel(b_ref, o_ref):
    total = b_ref[0]
    for k in range(1, b_ref.shape[0]):
        total = total + b_ref[k]
    for k in range(o_ref.shape[0]):
        o_ref[k] = total


def out(shape, dtype):
    return pltpu.VMEM(shape, dtype)


def body(acts, cotangent, depth_kernel, point_weight, gain, bias):
    n = lax.axis_size(SP)
    lines = lax.axis_size(LINE)
    copies = lax.axis_size(GRP)
    _, rows, cols, width = cotangent.shape
    places = rows * cols
    count = places * n
    half = -(-(-(-width // n) // 2) // 8) * 8
    g = cotangent[0]

    held = (g, depth_kernel, point_weight, gain[None], bias[None])
    near_g, near_k, near_w, gain, bias = call(
        stage_kernel, [out(a.shape, a.dtype) for a in held], "stage", 4 * width * width * 8, *held
    )
    x = lax.all_to_all(acts[:, 0], SP, 0, 0, tiled=True)
    d, p, stats = call(
        forward_kernel,
        [pltpu.HBM((places, width), BF), out((places, width), F32), out((n, 4, width), F32)],
        "forward", 2 * places * width * width, x, near_g, near_k, near_w,
    )
    stats = lax.all_to_all(stats, SP, 0, 0, tiled=True)
    (picked,) = call(
        lambda *refs: pick_kernel(n, *refs), [out((2 * n * half, places), BF)], "pick",
        4 * places * width * n * half, d, far=(0,),
    )
    coefs, dp, other = call(
        lambda *refs: project_kernel(float(count), *refs),
        [out((2, width), F32), out((places, width), BF), out((n, half, width), BF)],
        "project", 2 * places * width * n * half, stats, p, g, gain, picked,
    )
    other = lax.ppermute(other, "core", [(0, 1), (1, 0)])
    own, dinput, _ = call(
        input_kernel,
        [out((n * half, width), F32), out((rows, cols, width), BF), out((places, width), F32)],
        "input", 4 * places * width * width, dp, picked, point_weight, depth_kernel, g, x, far=(2,),
    )
    (packed,) = call(
        pack_kernel, [out((n, half + cols, width), BF)], "pack", n * half * width, own, other, dinput
    )
    packed = lax.all_to_all(packed, SP, 0, 0, tiled=True)
    (block_out,) = call(
        output_kernel, [out((rows, cols, width), BF)], "output", 4 * places * width,
        x, p, coefs, gain, bias,
    )
    each = -(-half // lines)
    (pieces,) = call(
        slice_kernel, [out((lines, each, width), F32)], "slice", n * half * width, packed
    )
    pieces = lax.all_to_all(pieces, LINE, 0, 0, tiled=True)
    (summed,) = call(
        copies_kernel, [out((copies, each, width), F32)], "copies", width * width, pieces
    )
    whole = lax.all_to_all(summed, GRP, 0, 0, tiled=True)
    whole = whole.reshape(lines, 2, each, width).swapaxes(1, 2).reshape(-1)
    span = width * width // n
    shift = (lax.axis_index(SP) * span) % width
    if (2 * span) % width == 0:
        odd = shift != 0
        weight_grad = jnp.where(odd, whole[width // 2 : width // 2 + span], whole[:span])
    else:
        weight_grad = lax.dynamic_slice(whole, (shift,), (span,))
    input_grad = packed[:, half:, :][:, None]
    return block_out[None], input_grad, weight_grad


def solution(mesh):
    sizes = (4, mesh.shape["grp"] // 8, 2, mesh.shape["sp"] // 2, 2)
    fine = Mesh(mesh.devices.reshape(sizes), ("yl", "z", "core", "x", "yh"))
    in_specs = (P(GRP, SP, None, None), P(GRP + SP, None, None, None), P(), P(), P(), P())
    out_specs = (P(GRP + SP, None, None, None), P(GRP, SP, None, None), P(SP))
    return jax.shard_map(body, mesh=fine, in_specs=in_specs, out_specs=out_specs, check_vma=False)
```

```python
import jax
import jax.numpy as jnp
import numpy as np
from jax import lax
from jax.experimental import pallas as pl
from jax.experimental.pallas import tpu as pltpu
from jax.sharding import Mesh, PartitionSpec as P

BF = jnp.bfloat16
F32 = jnp.float32
SP = ("x", "yh")
LINE = ("yl", "z")
GRP = ("yl", "z", "core")
VMEM = pl.BlockSpec(memory_space=pltpu.VMEM)


def held_in(a, space):
    return pltpu.with_memory_space_constraint(a, space)


def call(kernel, outs, flops, *args, far=()):
    size = sum(a.size * a.dtype.itemsize for a in args)
    size += sum(int(np.prod(o.shape)) * o.dtype.itemsize for o in outs)
    return pl.pallas_call(
        kernel,
        out_shape=outs,
        in_specs=[VMEM] * len(args),
        out_specs=[VMEM] * len(outs),
        cost_estimate=pl.CostEstimate(flops=flops, bytes_accessed=size, transcendentals=0),
        compiler_params=pltpu.CompilerParams(vmem_limit_bytes=16 * 2**20),
    )(*[held_in(a, pltpu.HBM if k in far else pltpu.VMEM) for k, a in enumerate(args)])


def spans(width, step):
    return [(a, min(a + step, width)) for a in range(0, width, step)]


def shifted(field):
    zero = jnp.zeros_like(field[:, :1, :])
    left = jnp.concatenate([zero, field[:, :-1, :]], axis=1)
    right = jnp.concatenate([field[:, 1:, :], zero], axis=1)
    return left, field, right


def nine_taps(field, taps, flip):
    rows = field.shape[0]
    near = shifted(field)
    out = []
    for r in range(rows):
        total = None
        for i in range(3):
            src = r + (1 - i if flip else i - 1)
            if src < 0 or src >= rows:
                continue
            for j in range(3):
                part = near[2 - j if flip else j][src] * taps[i, j : j + 1, :]
                total = part if total is None else total + part
        out.append(total)
    return out


def stage_kernel(*refs):
    half = len(refs) // 2
    for src, dst in zip(refs[:half], refs[half:]):
        dst[...] = src[...]


def forward_kernel(x_ref, g_ref, k_ref, w_ref, d_ref, p_ref, s_ref):
    rows, cols, width = x_ref.shape
    for a, b in spans(width, 128):
        h = jnp.maximum(x_ref[:, :, a:b].astype(F32), 0.0)
        for r, line in enumerate(nine_taps(h, k_ref[:, :, a:b], False)):
            d_ref[r * cols : (r + 1) * cols, a:b] = line.astype(BF)
    p_ref[...] = jnp.dot(d_ref[...], w_ref[...], preferred_element_type=F32)
    for a, b in spans(width, 128):
        p = p_ref[:, a:b]
        g = g_ref[:, :, a:b].astype(F32).reshape(rows * cols, b - a)
        sums = [jnp.sum(v, axis=0, keepdims=True) for v in (p, p * p, g, g * p)]
        stats = jnp.concatenate(sums, axis=0)
        for k in range(s_ref.shape[0]):
            s_ref[k, :, a:b] = stats


def pick_kernel(parts, d_ref, t_ref):
    width = d_ref.shape[1]
    lines = t_ref.shape[0]
    part = lines // 2 // parts
    per = -(-width // parts)
    core = lax.axis_index("core")
    line = lax.broadcasted_iota(jnp.int32, (lines, 1), 0)
    other = line >= lines // 2
    line = jnp.where(other, line - lines // 2, line)
    slot = (line * (65536 // part + 1)) >> 16
    row = 2 * (line - part * slot) + jnp.where(other, 1 - core, core)
    source = ((slot * (2 * width // parts)) >> 1) + row
    source = jnp.where(row < per, source, -1)
    chan = lax.broadcasted_iota(jnp.int32, (lines, width), 1)
    pick = jnp.where(chan == source, 1.0, 0.0).astype(BF)
    t = lax.dot_general(pick, d_ref[...], (((1,), (1,)), ((), ())), preferred_element_type=F32)
    t_ref[...] = t.astype(BF)


def project_kernel(count, s_ref, p_ref, g_ref, gain_ref, t_ref, c_ref, dp_ref, o_ref):
    rows, cols, width = g_ref.shape
    for a, b in spans(width, 128):
        stats = s_ref[0, :, a:b]
        for k in range(1, s_ref.shape[0]):
            stats = stats + s_ref[k, :, a:b]
        gain = gain_ref[:, a:b]
        mean = stats[0:1] / count
        var = stats[1:2] / count - mean * mean
        rstd = lax.rsqrt(var + 1e-05)
        lead = gain * stats[2:3] / count
        second = gain * rstd * (stats[3:4] - mean * stats[2:3]) / count
        c_ref[0:1, a:b] = mean
        c_ref[1:2, a:b] = rstd
        g = g_ref[:, :, a:b].astype(F32).reshape(rows * cols, b - a)
        xhat = (p_ref[:, a:b] - mean) * rstd
        dp_ref[:, a:b] = (rstd * (g * gain - lead - xhat * second)).astype(BF)
    half = t_ref.shape[0] // 2
    other = jnp.dot(t_ref[half:, :], dp_ref[...], preferred_element_type=F32).astype(BF)
    n, part, _ = o_ref.shape
    for k in range(n):
        o_ref[k] = other[k * part : (k + 1) * part, :]


def own_kernel(dp_ref, t_ref, m_ref):
    half = t_ref.shape[0] // 2
    m_ref[...] = jnp.dot(t_ref[:half, :], dp_ref[...], preferred_element_type=F32)


def input_kernel(dp_ref, w_ref, k_ref, g_ref, x_ref, keep_ref, send_ref, dd_ref):
    rows, cols, width = g_ref.shape
    low = lax.axis_index("yh") == 0
    dd_ref[...] = lax.dot_general(
        dp_ref[...], w_ref[...], (((1,), (1,)), ((), ())), preferred_element_type=F32
    )
    for a, b in spans(width, 128):
        dd = dd_ref[:, a:b].reshape(rows, cols, b - a)
        lines = []
        for r, line in enumerate(nine_taps(dd, k_ref[:, :, a:b], True)):
            kept = jnp.where(x_ref[r, :, a:b].astype(F32) > 0, line, 0.0)
            lines.append(g_ref[r, :, a:b].astype(F32) + kept)
        for r in range(rows // 2):
            even, odd = lines[2 * r], lines[2 * r + 1]
            keep_ref[r, :, a:b] = jnp.where(low, even, odd).astype(BF)
            send_ref[r, :, a:b] = jnp.where(low, odd, even).astype(BF)


def turn_kernel(keep_ref, got_ref, *out_refs):
    n = len(out_refs)
    me = lax.axis_index("x")
    low = lax.axis_index("yh") == 0
    for k, ref in enumerate(out_refs):
        to = lax.rem(me + k, n)
        keep = keep_ref[to].astype(F32)
        got = got_ref[to].astype(F32)
        ref[0] = jnp.where(low, keep, got).astype(BF)
        ref[1] = jnp.where(low, got, keep).astype(BF)


def place_kernel(*refs):
    o_ref = refs[-1]
    n = len(refs) - 1
    me = lax.axis_index("x")
    for k, ref in enumerate(refs[:-1]):
        at = 2 * lax.rem(me + n - k, n)
        o_ref[at] = ref[0]
        o_ref[at + 1] = ref[1]


def output_kernel(x_ref, p_ref, c_ref, gain_ref, bias_ref, o_ref):
    rows, cols, width = x_ref.shape
    for a, b in spans(width, 128):
        xhat = (p_ref[:, a:b] - c_ref[0:1, a:b]) * c_ref[1:2, a:b]
        norm = (gain_ref[:, a:b] * xhat).reshape(rows, cols, b - a)
        out = x_ref[:, :, a:b].astype(F32) + norm + bias_ref[:, a:b]
        o_ref[:, :, a:b] = out.astype(BF)


def pack_kernel(m_ref, r_ref, o_ref):
    n, part, _ = o_ref.shape
    for k in range(n):
        rows = slice(k * part, (k + 1) * part)
        o_ref[k] = (m_ref[rows, :] + r_ref[k].astype(F32)).astype(BF)


def slice_kernel(b_ref, o_ref):
    n = b_ref.shape[0]
    lines, per, width = o_ref.shape
    part = b_ref.shape[1]
    total = b_ref[0, :part, :].astype(F32)
    for k in range(1, n):
        total = total + b_ref[k, :part, :].astype(F32)
    for k in range(lines):
        for q in range(per):
            r = k * per + q
            if r < part:
                o_ref[k, q : q + 1, :] = total[r : r + 1, :]
            else:
                o_ref[k, q : q + 1, :] = jnp.zeros((1, width), F32)


def copies_kernel(b_ref, o_ref):
    total = b_ref[0]
    for k in range(1, b_ref.shape[0]):
        total = total + b_ref[k]
    for k in range(o_ref.shape[0]):
        o_ref[k] = total


def out(shape, dtype):
    return pltpu.VMEM(shape, dtype)


def body(acts, cotangent, depth_kernel, point_weight, gain, bias):
    n = lax.axis_size(SP)
    lines = lax.axis_size(LINE)
    copies = lax.axis_size(GRP)
    _, rows, cols, width = cotangent.shape
    places = rows * cols
    count = places * n
    half = -(-(-(-width // n) // 2) // 8) * 8
    g = cotangent[0]

    held = (g, depth_kernel, point_weight, gain[None], bias[None])
    near_g, near_k, near_w, gain, bias = call(
        stage_kernel, [out(a.shape, a.dtype) for a in held], 4 * width * width * 8, *held
    )
    x = lax.all_to_all(acts[:, 0], SP, 0, 0, tiled=True)
    d, p, stats = call(
        forward_kernel,
        [pltpu.HBM((places, width), BF), out((places, width), F32), out((n, 4, width), F32)],
        2 * places * width * width, x, near_g, near_k, near_w,
    )
    stats = lax.all_to_all(stats, SP, 0, 0, tiled=True)
    (picked,) = call(
        lambda *refs: pick_kernel(n, *refs), [out((2 * n * half, places), BF)],
        4 * places * width * n * half, d, far=(0,),
    )
    coefs, dp, other = call(
        lambda *refs: project_kernel(float(count), *refs),
        [out((2, width), F32), out((places, width), BF), out((n, half, width), BF)],
        2 * places * width * n * half, stats, p, g, gain, picked,
    )
    other = lax.ppermute(other, "core", [(0, 1), (1, 0)])
    (own,) = call(
        own_kernel, [out((n * half, width), F32)], 2 * places * width * n * half, dp, picked
    )
    (packed,) = call(pack_kernel, [out((n, half, width), BF)], n * half * width, own, other)
    packed = lax.all_to_all(packed, SP, 0, 0, tiled=True)
    keep, send, _ = call(
        input_kernel,
        [
            out((rows // 2, cols, width), BF),
            out((rows // 2, cols, width), BF),
            out((places, width), F32),
        ],
        4 * places * width * width, dp, point_weight, depth_kernel, g, x, far=(1,),
    )
    got = lax.ppermute(send, "yh", [(0, 1), (1, 0)])
    ring = lax.axis_size("x")
    turned = call(
        turn_kernel, [jax.ShapeDtypeStruct((2, cols, width), BF)] * ring,
        places * width, keep, got,
    )
    arrived = [turned[0]]
    for k in range(1, ring):
        pairs = [(i, (i + k) % ring) for i in range(ring)]
        arrived.append(lax.ppermute(turned[k], "x", pairs))
    (input_grad,) = call(
        place_kernel, [jax.ShapeDtypeStruct((rows, cols, width), BF)],
        places * width, *arrived,
    )
    input_grad = input_grad[:, None]
    (block_out,) = call(
        output_kernel, [out((rows, cols, width), BF)], 4 * places * width,
        x, p, coefs, gain, bias,
    )
    each = -(-half // lines)
    (pieces,) = call(slice_kernel, [out((lines, each, width), F32)], n * half * width, packed)
    pieces = lax.all_to_all(pieces, LINE, 0, 0, tiled=True)
    (summed,) = call(copies_kernel, [out((copies, each, width), F32)], width * width, pieces)
    whole = lax.all_to_all(summed, GRP, 0, 0, tiled=True)
    whole = whole.reshape(lines, 2, each, width).swapaxes(1, 2).reshape(-1)
    span = width * width // n
    shift = (lax.axis_index(SP) * span) % width
    if (2 * span) % width == 0:
        odd = shift != 0
        weight_grad = jnp.where(odd, whole[width // 2 : width // 2 + span], whole[:span])
    else:
        weight_grad = lax.dynamic_slice(whole, (shift,), (span,))
    return block_out[None], input_grad, weight_grad


def solution(mesh):
    sizes = (4, mesh.shape["grp"] // 8, 2, mesh.shape["sp"] // 2, 2)
    fine = Mesh(mesh.devices.reshape(sizes), ("yl", "z", "core", "x", "yh"))
    in_specs = (P(GRP, SP, None, None), P(GRP + SP, None, None, None), P(), P(), P(), P())
    out_specs = (P(GRP + SP, None, None, None), P(GRP, SP, None, None), P(SP))

    return jax.shard_map(body, mesh=fine, in_specs=in_specs, out_specs=out_specs, check_vma=False)
```

```python
import jax
import jax.numpy as jnp
import numpy as np
from jax import lax
from jax.experimental import pallas as pl
from jax.experimental.pallas import tpu as pltpu
from jax.sharding import Mesh, PartitionSpec as P

BF = jnp.bfloat16
F32 = jnp.float32
SP = ("x", "yh")
LINE = ("yl", "z")
GRP = ("yl", "z", "core")
VMEM = pl.BlockSpec(memory_space=pltpu.VMEM)


def held_in(a, space):
    return pltpu.with_memory_space_constraint(a, space)


def call(kernel, outs, name, flops, *args, far=()):
    size = sum(a.size * a.dtype.itemsize for a in args)
    size += sum(int(np.prod(o.shape)) * o.dtype.itemsize for o in outs)
    return pl.pallas_call(
        kernel,
        out_shape=outs,
        in_specs=[VMEM] * len(args),
        out_specs=[VMEM] * len(outs),
        cost_estimate=pl.CostEstimate(flops=flops, bytes_accessed=size, transcendentals=0),
        compiler_params=pltpu.CompilerParams(vmem_limit_bytes=16 * 2**20),
        name=name,
    )(*[held_in(a, pltpu.HBM if k in far else pltpu.VMEM) for k, a in enumerate(args)])


def spans(width, step):
    return [(a, min(a + step, width)) for a in range(0, width, step)]


def shifted(field):
    zero = jnp.zeros_like(field[:, :1, :])
    left = jnp.concatenate([zero, field[:, :-1, :]], axis=1)
    right = jnp.concatenate([field[:, 1:, :], zero], axis=1)
    return left, field, right


def nine_taps(field, taps, flip):
    rows = field.shape[0]
    near = shifted(field)
    out = []
    for r in range(rows):
        total = None
        for i in range(3):
            src = r + (1 - i if flip else i - 1)
            if src < 0 or src >= rows:
                continue
            for j in range(3):
                part = near[2 - j if flip else j][src] * taps[i, j : j + 1, :]
                total = part if total is None else total + part
        out.append(total)
    return out


def stage_kernel(*refs):
    half = len(refs) // 2
    for src, dst in zip(refs[:half], refs[half:]):
        dst[...] = src[...]


def forward_kernel(x_ref, g_ref, k_ref, w_ref, d_ref, p_ref, s_ref):
    rows, cols, width = x_ref.shape
    for a, b in spans(width, 128):
        h = jnp.maximum(x_ref[:, :, a:b].astype(F32), 0.0)
        for r, line in enumerate(nine_taps(h, k_ref[:, :, a:b], False)):
            d_ref[r * cols : (r + 1) * cols, a:b] = line.astype(BF)
    p_ref[...] = jnp.dot(d_ref[...], w_ref[...], preferred_element_type=F32)
    for a, b in spans(width, 128):
        p = p_ref[:, a:b]
        g = g_ref[:, :, a:b].astype(F32).reshape(rows * cols, b - a)
        sums = [jnp.sum(v, axis=0, keepdims=True) for v in (p, p * p, g, g * p)]
        stats = jnp.concatenate(sums, axis=0)
        for k in range(s_ref.shape[0]):
            s_ref[k, :, a:b] = stats


def pick_kernel(parts, d_ref, t_ref):
    width = d_ref.shape[1]
    lines = t_ref.shape[0]
    part = lines // 2 // parts
    per = -(-width // parts)
    core = lax.axis_index("core")
    line = lax.broadcasted_iota(jnp.int32, (lines, 1), 0)
    other = line >= lines // 2
    line = jnp.where(other, line - lines // 2, line)
    slot = (line * (65536 // part + 1)) >> 16
    row = 2 * (line - part * slot) + jnp.where(other, 1 - core, core)
    source = ((slot * (2 * width // parts)) >> 1) + row
    source = jnp.where(row < per, source, -1)
    chan = lax.broadcasted_iota(jnp.int32, (lines, width), 1)
    pick = jnp.where(chan == source, 1.0, 0.0).astype(BF)
    t = lax.dot_general(pick, d_ref[...], (((1,), (1,)), ((), ())), preferred_element_type=F32)
    t_ref[...] = t.astype(BF)


def project_kernel(count, s_ref, p_ref, g_ref, gain_ref, t_ref, c_ref, dp_ref, o_ref):
    rows, cols, width = g_ref.shape
    for a, b in spans(width, 128):
        stats = s_ref[0, :, a:b]
        for k in range(1, s_ref.shape[0]):
            stats = stats + s_ref[k, :, a:b]
        gain = gain_ref[:, a:b]
        mean = stats[0:1] / count
        var = stats[1:2] / count - mean * mean
        rstd = lax.rsqrt(var + 1e-05)
        lead = gain * stats[2:3] / count
        second = gain * rstd * (stats[3:4] - mean * stats[2:3]) / count
        c_ref[0:1, a:b] = mean
        c_ref[1:2, a:b] = rstd
        g = g_ref[:, :, a:b].astype(F32).reshape(rows * cols, b - a)
        xhat = (p_ref[:, a:b] - mean) * rstd
        dp_ref[:, a:b] = (rstd * (g * gain - lead - xhat * second)).astype(BF)
    half = t_ref.shape[0] // 2
    other = jnp.dot(t_ref[half:, :], dp_ref[...], preferred_element_type=F32).astype(BF)
    n, part, _ = o_ref.shape
    for k in range(n):
        o_ref[k] = other[k * part : (k + 1) * part, :]


def input_kernel(dp_ref, t_ref, w_ref, k_ref, g_ref, x_ref, m_ref, di_ref, dd_ref):
    rows, cols, width = g_ref.shape
    half = t_ref.shape[0] // 2
    m_ref[...] = jnp.dot(t_ref[:half, :], dp_ref[...], preferred_element_type=F32)
    dd_ref[...] = lax.dot_general(
        dp_ref[...], w_ref[...], (((1,), (1,)), ((), ())), preferred_element_type=F32
    )
    for a, b in spans(width, 128):
        dd = dd_ref[:, a:b].reshape(rows, cols, b - a)
        for r, line in enumerate(nine_taps(dd, k_ref[:, :, a:b], True)):
            kept = jnp.where(x_ref[r, :, a:b].astype(F32) > 0, line, 0.0)
            di_ref[r, :, a:b] = (g_ref[r, :, a:b].astype(F32) + kept).astype(BF)


def output_kernel(x_ref, p_ref, c_ref, gain_ref, bias_ref, o_ref):
    rows, cols, width = x_ref.shape
    for a, b in spans(width, 128):
        xhat = (p_ref[:, a:b] - c_ref[0:1, a:b]) * c_ref[1:2, a:b]
        norm = (gain_ref[:, a:b] * xhat).reshape(rows, cols, b - a)
        out = x_ref[:, :, a:b].astype(F32) + norm + bias_ref[:, a:b]
        o_ref[:, :, a:b] = out.astype(BF)


def pack_kernel(m_ref, r_ref, di_ref, o_ref):
    n, cols, _ = di_ref.shape
    part = m_ref.shape[0] // n
    for k in range(n):
        rows = slice(k * part, (k + 1) * part)
        o_ref[k, :part, :] = (m_ref[rows, :] + r_ref[k].astype(F32)).astype(BF)
        o_ref[k, part:, :] = di_ref[k]


def slice_kernel(b_ref, o_ref):
    n = b_ref.shape[0]
    lines, per, width = o_ref.shape
    part = b_ref.shape[1] - 16
    total = b_ref[0, :part, :].astype(F32)
    for k in range(1, n):
        total = total + b_ref[k, :part, :].astype(F32)
    for k in range(lines):
        for q in range(per):
            r = k * per + q
            if r < part:
                o_ref[k, q : q + 1, :] = total[r : r + 1, :]
            else:
                o_ref[k, q : q + 1, :] = jnp.zeros((1, width), F32)


def copies_kernel(b_ref, o_ref):
    total = b_ref[0]
    for k in range(1, b_ref.shape[0]):
        total = total + b_ref[k]
    for k in range(o_ref.shape[0]):
        o_ref[k] = total


def final_kernel(b_ref, o_ref):
    span = o_ref.shape[0]
    width = b_ref.shape[-1]
    odd = lax.rem(lax.axis_index("yh"), 2) == 1
    half = width // 2
    each = b_ref.shape[1]

    def row_at(r):
        q = r // 2 % each
        return b_ref[r // 2 // each * 2 + r % 2, q : q + 1, :]

    for r in range(-(-span // width)):
        row = row_at(r)
        after = row_at(r + 1)
        late = jnp.concatenate([row[:, half:], after[:, :half]], axis=1)
        line = jnp.where(odd, late, row).reshape(width)
        size = min(width, span - r * width)
        o_ref[r * width : r * width + size] = line[:size]


def out(shape, dtype):
    return pltpu.VMEM(shape, dtype)


def body(acts, cotangent, depth_kernel, point_weight, gain, bias):
    n = lax.axis_size(SP)
    lines = lax.axis_size(LINE)
    copies = lax.axis_size(GRP)
    _, rows, cols, width = cotangent.shape
    places = rows * cols
    count = places * n
    half = -(-(-(-width // n) // 2) // 8) * 8
    g = cotangent[0]

    held = (g, depth_kernel, point_weight, gain[None], bias[None])
    near_g, near_k, near_w, gain, bias = call(
        stage_kernel, [out(a.shape, a.dtype) for a in held], "stage", 4 * width * width * 8, *held
    )
    x = lax.all_to_all(acts[:, 0], SP, 0, 0, tiled=True)
    d, p, stats = call(
        forward_kernel,
        [pltpu.HBM((places, width), BF), out((places, width), F32), out((n, 4, width), F32)],
        "forward", 2 * places * width * width, x, near_g, near_k, near_w,
    )
    stats = lax.all_to_all(stats, SP, 0, 0, tiled=True)
    (picked,) = call(
        lambda *refs: pick_kernel(n, *refs), [out((2 * n * half, places), BF)], "pick",
        4 * places * width * n * half, d, far=(0,),
    )
    coefs, dp, other = call(
        lambda *refs: project_kernel(float(count), *refs),
        [out((2, width), F32), out((places, width), BF), out((n, half, width), BF)],
        "project", 2 * places * width * n * half, stats, p, g, gain, picked,
    )
    other = lax.ppermute(other, "core", [(0, 1), (1, 0)])
    own, dinput, _ = call(
        input_kernel,
        [out((n * half, width), F32), out((rows, cols, width), BF), out((places, width), F32)],
        "input", 4 * places * width * width, dp, picked, point_weight, depth_kernel, g, x,
    )
    (packed,) = call(
        pack_kernel, [out((n, half + cols, width), BF)], "pack", n * half * width, own, other, dinput
    )
    packed = lax.all_to_all(packed, SP, 0, 0, tiled=True)
    (block_out,) = call(
        output_kernel, [out((rows, cols, width), BF)], "output", 4 * places * width,
        x, p, coefs, gain, bias,
    )
    each = -(-half // lines)
    (pieces,) = call(
        slice_kernel, [out((lines, each, width), F32)], "slice", n * half * width, packed
    )
    pieces = lax.all_to_all(pieces, LINE, 0, 0, tiled=True)
    (summed,) = call(
        copies_kernel, [out((copies, each, width), F32)], "copies", width * width, pieces
    )
    whole = lax.all_to_all(summed, GRP, 0, 0, tiled=True)
    (weight_grad,) = call(
        final_kernel, [jax.ShapeDtypeStruct((width * width // n,), F32)], "final", width * width,
        whole,
    )
    input_grad = packed[:, half:, :][:, None]
    return block_out[None], input_grad, weight_grad


def solution(mesh):
    sizes = (4, mesh.shape["grp"] // 8, 2, mesh.shape["sp"] // 2, 2)
    fine = Mesh(mesh.devices.reshape(sizes), ("yl", "z", "core", "x", "yh"))
    in_specs = (P(GRP, SP, None, None), P(GRP + SP, None, None, None), P(), P(), P(), P())
    out_specs = (P(GRP + SP, None, None, None), P(GRP, SP, None, None), P(SP))
    return jax.shard_map(body, mesh=fine, in_specs=in_specs, out_specs=out_specs, check_vma=False)
```

```python
import jax
import jax.numpy as jnp
import numpy as np
from jax import lax
from jax.experimental import pallas as pl
from jax.experimental.pallas import tpu as pltpu
from jax.sharding import Mesh, PartitionSpec as P

BF = jnp.bfloat16
F32 = jnp.float32
SP = ("x", "yh")
LINE = ("yl", "z")
GRP = ("yl", "z", "core")
PAIR = ("z", "core")
VMEM = pl.BlockSpec(memory_space=pltpu.VMEM)


def held_in(a, space):
    return pltpu.with_memory_space_constraint(a, space)


def call(kernel, outs, name, flops, *args, far=()):
    size = sum(a.size * a.dtype.itemsize for a in args)
    size += sum(int(np.prod(o.shape)) * o.dtype.itemsize for o in outs)
    return pl.pallas_call(
        kernel,
        out_shape=outs,
        in_specs=[VMEM] * len(args),
        out_specs=[VMEM] * len(outs),
        cost_estimate=pl.CostEstimate(flops=flops, bytes_accessed=size, transcendentals=0),
        compiler_params=pltpu.CompilerParams(vmem_limit_bytes=16 * 2**20),
        name=name,
    )(*[held_in(a, pltpu.HBM if k in far else pltpu.VMEM) for k, a in enumerate(args)])


def spans(width, step):
    return [(a, min(a + step, width)) for a in range(0, width, step)]


def shifted(field):
    zero = jnp.zeros_like(field[:, :1, :])
    left = jnp.concatenate([zero, field[:, :-1, :]], axis=1)
    right = jnp.concatenate([field[:, 1:, :], zero], axis=1)
    return left, field, right


def nine_taps(field, taps, flip):
    rows = field.shape[0]
    near = shifted(field)
    out = []
    for r in range(rows):
        total = None
        for i in range(3):
            src = r + (1 - i if flip else i - 1)
            if src < 0 or src >= rows:
                continue
            for j in range(3):
                part = near[2 - j if flip else j][src] * taps[i, j : j + 1, :]
                total = part if total is None else total + part
        out.append(total)
    return out


def stage_kernel(*refs):
    half = len(refs) // 2
    for src, dst in zip(refs[:half], refs[half:]):
        dst[...] = src[...]


def forward_kernel(x_ref, g_ref, k_ref, w_ref, d_ref, p_ref, s_ref):
    rows, cols, width = x_ref.shape
    for a, b in spans(width, 128):
        h = jnp.maximum(x_ref[:, :, a:b].astype(F32), 0.0)
        for r, line in enumerate(nine_taps(h, k_ref[:, :, a:b], False)):
            d_ref[r * cols : (r + 1) * cols, a:b] = line.astype(BF)
    p_ref[...] = jnp.dot(d_ref[...], w_ref[...], preferred_element_type=F32)
    for a, b in spans(width, 128):
        p = p_ref[:, a:b]
        g = g_ref[:, :, a:b].astype(F32).reshape(rows * cols, b - a)
        sums = [jnp.sum(v, axis=0, keepdims=True) for v in (p, p * p, g, g * p)]
        stats = jnp.concatenate(sums, axis=0)
        for k in range(s_ref.shape[0]):
            s_ref[k, :, a:b] = stats


def pick_kernel(parts, each, d_ref, t_ref):
    width = d_ref.shape[1]
    lines = t_ref.shape[0]
    part = lines // 2 // parts
    per = -(-width // parts)
    core = lax.axis_index("core")
    line = lax.broadcasted_iota(jnp.int32, (lines, 1), 0)
    other = line >= lines // 2
    line = jnp.where(other, line - lines // 2, line)
    slot = (line * (65536 // part + 1)) >> 16
    inner = line - part * slot
    block = (inner * (65536 // each + 1)) >> 16
    row = inner + each * (block + jnp.where(other, 1 - core, core))
    source = ((slot * (2 * width // parts)) >> 1) + row
    source = jnp.where(row < per, source, -1)
    chan = lax.broadcasted_iota(jnp.int32, (lines, width), 1)
    pick = jnp.where(chan == source, 1.0, 0.0).astype(BF)
    t = lax.dot_general(pick, d_ref[...], (((1,), (1,)), ((), ())), preferred_element_type=F32)
    t_ref[...] = t.astype(BF)


def project_kernel(count, s_ref, p_ref, g_ref, gain_ref, t_ref, c_ref, dp_ref, o_ref):
    rows, cols, width = g_ref.shape
    for a, b in spans(width, 128):
        stats = s_ref[0, :, a:b]
        for k in range(1, s_ref.shape[0]):
            stats = stats + s_ref[k, :, a:b]
        gain = gain_ref[:, a:b]
        mean = stats[0:1] / count
        var = stats[1:2] / count - mean * mean
        rstd = lax.rsqrt(var + 1e-05)
        lead = gain * stats[2:3] / count
        second = gain * rstd * (stats[3:4] - mean * stats[2:3]) / count
        c_ref[0:1, a:b] = mean
        c_ref[1:2, a:b] = rstd
        g = g_ref[:, :, a:b].astype(F32).reshape(rows * cols, b - a)
        xhat = (p_ref[:, a:b] - mean) * rstd
        dp_ref[:, a:b] = (rstd * (g * gain - lead - xhat * second)).astype(BF)
    half = t_ref.shape[0] // 2
    other = jnp.dot(t_ref[half:, :], dp_ref[...], preferred_element_type=F32).astype(BF)
    n, part, _ = o_ref.shape
    for k in range(n):
        o_ref[k] = other[k * part : (k + 1) * part, :]


def input_kernel(dp_ref, t_ref, w_ref, k_ref, g_ref, x_ref, m_ref, di_ref, dd_ref):
    rows, cols, width = g_ref.shape
    half = t_ref.shape[0] // 2
    m_ref[...] = jnp.dot(t_ref[:half, :], dp_ref[...], preferred_element_type=F32)
    dd_ref[...] = lax.dot_general(
        dp_ref[...], w_ref[...], (((1,), (1,)), ((), ())), preferred_element_type=F32
    )
    for a, b in spans(width, 128):
        dd = dd_ref[:, a:b].reshape(rows, cols, b - a)
        for r, line in enumerate(nine_taps(dd, k_ref[:, :, a:b], True)):
            kept = jnp.where(x_ref[r, :, a:b].astype(F32) > 0, line, 0.0)
            di_ref[r, :, a:b] = (g_ref[r, :, a:b].astype(F32) + kept).astype(BF)


def output_kernel(x_ref, p_ref, c_ref, gain_ref, bias_ref, o_ref):
    rows, cols, width = x_ref.shape
    for a, b in spans(width, 128):
        xhat = (p_ref[:, a:b] - c_ref[0:1, a:b]) * c_ref[1:2, a:b]
        norm = (gain_ref[:, a:b] * xhat).reshape(rows, cols, b - a)
        out = x_ref[:, :, a:b].astype(F32) + norm + bias_ref[:, a:b]
        o_ref[:, :, a:b] = out.astype(BF)


def pack_kernel(m_ref, r_ref, di_ref, o_ref):
    n, cols, _ = di_ref.shape
    part = m_ref.shape[0] // n
    for k in range(n):
        rows = slice(k * part, (k + 1) * part)
        o_ref[k, :part, :] = (m_ref[rows, :] + r_ref[k].astype(F32)).astype(BF)
        o_ref[k, part:, :] = di_ref[k]


def slice_kernel(b_ref, o_ref):
    n = b_ref.shape[0]
    lines, per, width = o_ref.shape
    part = b_ref.shape[1] - 16
    total = b_ref[0, :part, :].astype(F32)
    for k in range(1, n):
        total = total + b_ref[k, :part, :].astype(F32)
    for k in range(lines):
        at = k % (part // per) * per
        o_ref[k] = total[at : at + per, :].astype(BF)


def copies_kernel(b_ref, o_ref):
    total = b_ref[0].astype(F32)
    for k in range(1, b_ref.shape[0]):
        total = total + b_ref[k].astype(F32)
    for k in range(o_ref.shape[0]):
        o_ref[k] = total


def out(shape, dtype):
    return pltpu.VMEM(shape, dtype)


def body(acts, cotangent, depth_kernel, point_weight, gain, bias):
    n = lax.axis_size(SP)
    lines = lax.axis_size(LINE)
    _, rows, cols, width = cotangent.shape
    places = rows * cols
    count = places * n
    half = -(-(-(-width // n) // 2) // 8) * 8
    blocks = lax.axis_size("z")
    each = half // blocks
    g = cotangent[0]

    held = (g, depth_kernel, point_weight, gain[None], bias[None])
    near_g, near_k, near_w, gain, bias = call(
        stage_kernel, [out(a.shape, a.dtype) for a in held], "stage", 4 * width * width * 8, *held
    )
    x = lax.all_to_all(acts[:, 0], SP, 0, 0, tiled=True)
    d, p, stats = call(
        forward_kernel,
        [pltpu.HBM((places, width), BF), out((places, width), F32), out((n, 4, width), F32)],
        "forward", 2 * places * width * width, x, near_g, near_k, near_w,
    )
    stats = lax.all_to_all(stats, SP, 0, 0, tiled=True)
    (picked,) = call(
        lambda *refs: pick_kernel(n, each, *refs), [out((2 * n * half, places), BF)], "pick",
        4 * places * width * n * half, d, far=(0,),
    )
    coefs, dp, other = call(
        lambda *refs: project_kernel(float(count), *refs),
        [out((2, width), F32), out((places, width), BF), out((n, half, width), BF)],
        "project", 2 * places * width * n * half, stats, p, g, gain, picked,
    )
    other = lax.ppermute(other, "core", [(0, 1), (1, 0)])
    own, dinput, _ = call(
        input_kernel,
        [out((n * half, width), F32), out((rows, cols, width), BF), out((places, width), F32)],
        "input", 4 * places * width * width, dp, picked, point_weight, depth_kernel, g, x,
    )
    (packed,) = call(
        pack_kernel, [out((n, half + cols, width), BF)], "pack", n * half * width, own, other, dinput
    )
    packed = lax.all_to_all(packed, SP, 0, 0, tiled=True)
    (block_out,) = call(
        output_kernel, [out((rows, cols, width), BF)], "output", 4 * places * width,
        x, p, coefs, gain, bias,
    )
    (pieces,) = call(
        slice_kernel, [out((lines, each, width), BF)], "slice", n * half * width, packed
    )
    pieces = lax.all_to_all(pieces, LINE, 0, 0, tiled=True)
    (summed,) = call(
        copies_kernel, [out((2 * blocks, each, width), F32)], "copies", width * width, pieces
    )
    whole = lax.all_to_all(summed, PAIR, 0, 0, tiled=True)
    whole = whole.reshape(-1)
    span = width * width // n
    shift = (lax.axis_index(SP) * span) % width
    if (2 * span) % width == 0:
        odd = shift != 0
        weight_grad = jnp.where(odd, whole[width // 2 : width // 2 + span], whole[:span])
    else:
        weight_grad = lax.dynamic_slice(whole, (shift,), (span,))
    input_grad = packed[:, half:, :][:, None]
    return block_out[None], input_grad, weight_grad


def solution(mesh):
    sizes = (4, mesh.shape["grp"] // 8, 2, mesh.shape["sp"] // 2, 2)
    fine = Mesh(mesh.devices.reshape(sizes), ("yl", "z", "core", "x", "yh"))
    in_specs = (P(GRP, SP, None, None), P(GRP + SP, None, None, None), P(), P(), P(), P())
    out_specs = (P(GRP + SP, None, None, None), P(GRP, SP, None, None), P(SP))
    return jax.shard_map(body, mesh=fine, in_specs=in_specs, out_specs=out_specs, check_vma=False)
```

```python
import jax
import jax.numpy as jnp
import numpy as np
from jax import lax
from jax.experimental import pallas as pl
from jax.experimental.pallas import tpu as pltpu
from jax.sharding import Mesh, PartitionSpec as P

BF = jnp.bfloat16
F32 = jnp.float32
SP = ("x", "yh")
LINE = ("yl", "z")
GRP = ("yl", "z", "core")
PAIR = ("z", "core")
VMEM = pl.BlockSpec(memory_space=pltpu.VMEM)


def held_in(a, space):
    return pltpu.with_memory_space_constraint(a, space)


def call(kernel, outs, name, flops, *args, far=()):
    size = sum(a.size * a.dtype.itemsize for a in args)
    size += sum(int(np.prod(o.shape)) * o.dtype.itemsize for o in outs)
    return pl.pallas_call(
        kernel,
        out_shape=outs,
        in_specs=[VMEM] * len(args),
        out_specs=[VMEM] * len(outs),
        cost_estimate=pl.CostEstimate(flops=flops, bytes_accessed=size, transcendentals=0),
        compiler_params=pltpu.CompilerParams(vmem_limit_bytes=16 * 2**20),
        name=name,
    )(*[held_in(a, pltpu.HBM if k in far else pltpu.VMEM) for k, a in enumerate(args)])


def spans(width, step):
    return [(a, min(a + step, width)) for a in range(0, width, step)]


def shifted(field):
    zero = jnp.zeros_like(field[:, :1, :])
    left = jnp.concatenate([zero, field[:, :-1, :]], axis=1)
    right = jnp.concatenate([field[:, 1:, :], zero], axis=1)
    return left, field, right


def nine_taps(field, taps, flip):
    rows = field.shape[0]
    near = shifted(field)
    out = []
    for r in range(rows):
        total = None
        for i in range(3):
            src = r + (1 - i if flip else i - 1)
            if src < 0 or src >= rows:
                continue
            for j in range(3):
                part = near[2 - j if flip else j][src] * taps[i, j : j + 1, :]
                total = part if total is None else total + part
        out.append(total)
    return out


def stage_kernel(*refs):
    half = len(refs) // 2
    for src, dst in zip(refs[:half], refs[half:]):
        dst[...] = src[...]


def forward_kernel(x_ref, g_ref, k_ref, w_ref, d_ref, p_ref, s_ref):
    rows, cols, width = x_ref.shape
    for a, b in spans(width, 128):
        h = jnp.maximum(x_ref[:, :, a:b].astype(F32), 0.0)
        for r, line in enumerate(nine_taps(h, k_ref[:, :, a:b], False)):
            d_ref[r * cols : (r + 1) * cols, a:b] = line.astype(BF)
    p_ref[...] = jnp.dot(d_ref[...], w_ref[...], preferred_element_type=F32)
    for a, b in spans(width, 128):
        p = p_ref[:, a:b]
        g = g_ref[:, :, a:b].astype(F32).reshape(rows * cols, b - a)
        sums = [jnp.sum(v, axis=0, keepdims=True) for v in (p, p * p, g, g * p)]
        stats = jnp.concatenate(sums, axis=0)
        for k in range(s_ref.shape[0]):
            s_ref[k, :, a:b] = stats


def pick_kernel(parts, each, d_ref, t_ref):
    width = d_ref.shape[1]
    lines = t_ref.shape[0]
    part = lines // 2 // parts
    per = -(-width // parts)
    core = lax.axis_index("core")
    line = lax.broadcasted_iota(jnp.int32, (lines, 1), 0)
    other = line >= lines // 2
    line = jnp.where(other, line - lines // 2, line)
    slot = (line * (65536 // part + 1)) >> 16
    inner = line - part * slot
    block = (inner * (65536 // each + 1)) >> 16
    row = inner + each * (block + jnp.where(other, 1 - core, core))
    source = ((slot * (2 * width // parts)) >> 1) + row
    source = jnp.where(row < per, source, -1)
    chan = lax.broadcasted_iota(jnp.int32, (lines, width), 1)
    pick = jnp.where(chan == source, 1.0, 0.0).astype(BF)
    t = lax.dot_general(pick, d_ref[...], (((1,), (1,)), ((), ())), preferred_element_type=F32)
    t_ref[...] = t.astype(BF)


def project_kernel(count, s_ref, p_ref, g_ref, gain_ref, t_ref, c_ref, dp_ref, o_ref):
    rows, cols, width = g_ref.shape
    for a, b in spans(width, 128):
        stats = s_ref[0, :, a:b]
        for k in range(1, s_ref.shape[0]):
            stats = stats + s_ref[k, :, a:b]
        gain = gain_ref[:, a:b]
        mean = stats[0:1] / count
        var = stats[1:2] / count - mean * mean
        rstd = lax.rsqrt(var + 1e-05)
        lead = gain * stats[2:3] / count
        second = gain * rstd * (stats[3:4] - mean * stats[2:3]) / count
        c_ref[0:1, a:b] = mean
        c_ref[1:2, a:b] = rstd
        g = g_ref[:, :, a:b].astype(F32).reshape(rows * cols, b - a)
        xhat = (p_ref[:, a:b] - mean) * rstd
        dp_ref[:, a:b] = (rstd * (g * gain - lead - xhat * second)).astype(BF)
    half = t_ref.shape[0] // 2
    other = jnp.dot(t_ref[half:, :], dp_ref[...], preferred_element_type=F32).astype(BF)
    n, part, _ = o_ref.shape
    for k in range(n):
        o_ref[k] = other[k * part : (k + 1) * part, :]


def input_kernel(dp_ref, t_ref, w_ref, k_ref, g_ref, x_ref, m_ref, di_ref, dd_ref):
    rows, cols, width = g_ref.shape
    half = t_ref.shape[0] // 2
    m_ref[...] = jnp.dot(t_ref[:half, :], dp_ref[...], preferred_element_type=F32)
    dd_ref[...] = lax.dot_general(
        dp_ref[...], w_ref[...], (((1,), (1,)), ((), ())), preferred_element_type=F32
    )
    for a, b in spans(width, 128):
        dd = dd_ref[:, a:b].reshape(rows, cols, b - a)
        for r, line in enumerate(nine_taps(dd, k_ref[:, :, a:b], True)):
            kept = jnp.where(x_ref[r, :, a:b].astype(F32) > 0, line, 0.0)
            di_ref[r, :, a:b] = (g_ref[r, :, a:b].astype(F32) + kept).astype(BF)


def output_kernel(x_ref, p_ref, c_ref, gain_ref, bias_ref, o_ref):
    rows, cols, width = x_ref.shape
    for a, b in spans(width, 128):
        xhat = (p_ref[:, a:b] - c_ref[0:1, a:b]) * c_ref[1:2, a:b]
        norm = (gain_ref[:, a:b] * xhat).reshape(rows, cols, b - a)
        out = x_ref[:, :, a:b].astype(F32) + norm + bias_ref[:, a:b]
        o_ref[:, :, a:b] = out.astype(BF)


def pack_kernel(m_ref, r_ref, di_ref, o_ref):
    n, cols, _ = di_ref.shape
    part = m_ref.shape[0] // n
    for k in range(n):
        rows = slice(k * part, (k + 1) * part)
        o_ref[k, :part, :] = (m_ref[rows, :] + r_ref[k].astype(F32)).astype(BF)
        o_ref[k, part:, :] = di_ref[k]


def slice_kernel(b_ref, o_ref):
    n = b_ref.shape[0]
    lines, per, width = o_ref.shape
    part = b_ref.shape[1] - 16
    total = b_ref[0, :part, :].astype(F32)
    for k in range(1, n):
        total = total + b_ref[k, :part, :].astype(F32)
    for k in range(lines):
        at = k % (part // per) * per
        o_ref[k] = total[at : at + per, :].astype(BF)


def copies_kernel(b_ref, o_ref):
    total = b_ref[0].astype(F32)
    for k in range(1, b_ref.shape[0]):
        total = total + b_ref[k].astype(F32)
    total = total.astype(BF)
    for k in range(o_ref.shape[0]):
        o_ref[k] = total


def finish_kernel(b_ref, o_ref):
    n, _, width = b_ref.shape
    half = width // 2
    odd = lax.axis_index("yh") == 1
    rows = jnp.concatenate([b_ref[k].astype(F32) for k in range(n)], axis=0)
    after = jnp.concatenate([rows[1:], rows[:1]], axis=0)
    late = jnp.concatenate([rows[:, half:], after[:, :half]], axis=1)
    o_ref[...] = jnp.where(odd, late, rows)


def out(shape, dtype):
    return pltpu.VMEM(shape, dtype)


def body(acts, cotangent, depth_kernel, point_weight, gain, bias):
    n = lax.axis_size(SP)
    lines = lax.axis_size(LINE)
    _, rows, cols, width = cotangent.shape
    places = rows * cols
    count = places * n
    half = -(-(-(-width // n) // 2) // 8) * 8
    blocks = lax.axis_size("z")
    each = half // blocks
    g = cotangent[0]

    held = (g, depth_kernel, point_weight, gain[None], bias[None])
    near_g, near_k, near_w, gain, bias = call(
        stage_kernel, [out(a.shape, a.dtype) for a in held], "stage", 4 * width * width * 8, *held
    )
    x = lax.all_to_all(acts[:, 0], SP, 0, 0, tiled=True)
    d, p, stats = call(
        forward_kernel,
        [pltpu.HBM((places, width), BF), out((places, width), F32), out((n, 4, width), F32)],
        "forward", 2 * places * width * width, x, near_g, near_k, near_w,
    )
    stats = lax.all_to_all(stats, SP, 0, 0, tiled=True)
    (picked,) = call(
        lambda *refs: pick_kernel(n, each, *refs), [out((2 * n * half, places), BF)], "pick",
        4 * places * width * n * half, d, far=(0,),
    )
    coefs, dp, other = call(
        lambda *refs: project_kernel(float(count), *refs),
        [out((2, width), F32), out((places, width), BF), out((n, half, width), BF)],
        "project", 2 * places * width * n * half, stats, p, g, gain, picked,
    )
    other = lax.ppermute(other, "core", [(0, 1), (1, 0)])
    own, dinput, _ = call(
        input_kernel,
        [out((n * half, width), F32), out((rows, cols, width), BF), out((places, width), F32)],
        "input", 4 * places * width * width, dp, picked, point_weight, depth_kernel, g, x,
    )
    (packed,) = call(
        pack_kernel, [out((n, half + cols, width), BF)], "pack", n * half * width, own, other, dinput
    )
    packed = lax.all_to_all(packed, SP, 0, 0, tiled=True)
    (block_out,) = call(
        output_kernel, [out((rows, cols, width), BF)], "output", 4 * places * width,
        x, p, coefs, gain, bias,
    )
    (pieces,) = call(
        slice_kernel, [out((lines, each, width), BF)], "slice", n * half * width, packed
    )
    pieces = lax.all_to_all(pieces, LINE, 0, 0, tiled=True)
    (summed,) = call(
        copies_kernel, [out((2 * blocks, each, width), BF)], "copies", width * width, pieces
    )
    whole = lax.all_to_all(summed, PAIR, 0, 0, tiled=True)
    (lined,) = call(
        finish_kernel, [out((2 * half, width), F32)], "finish", width * width, whole
    )
    weight_grad = lined.reshape(-1)[: width * width // n]
    input_grad = packed[:, half:, :][:, None]
    return block_out[None], input_grad, weight_grad


def solution(mesh):
    sizes = (4, mesh.shape["grp"] // 8, 2, mesh.shape["sp"] // 2, 2)
    fine = Mesh(mesh.devices.reshape(sizes), ("yl", "z", "core", "x", "yh"))
    in_specs = (P(GRP, SP, None, None), P(GRP + SP, None, None, None), P(), P(), P(), P())
    out_specs = (P(GRP + SP, None, None, None), P(GRP, SP, None, None), P(SP))
    return jax.shard_map(body, mesh=fine, in_specs=in_specs, out_specs=out_specs, check_vma=False)
```
